1024 devices in a mesh: fsdp: 16 (over z_lo, core), roll: 64 (over y, z_hi, x).
Axes of the slice: x: 4, y: 8, z: 16 (z_hi: 2, z_lo: 8; z = z_hi * 8 + z_lo), core: 2. Of those that a mesh axis runs over, the one named last changes fastest.
Arguments:
- trainer_weights: bfloat16 [64, 1024, 8192], P('roll', None, 'fsdp'), may hold values from -0.09375 to 0.09375
- power_table: int32 [8192, 512], P('fsdp'), may hold values from 1 to 250, as said below
- assign: int32 [2], replicated, may hold values from 0 to 63
Outputs:
- rollout_weights: bfloat16 [64, 2, 1024, 8192], P('roll', None, 'fsdp')
- fingerprint: bfloat16 [64, 2, 1024, 512], P('roll', None, 'fsdp')
The draws below stay inside these ranges and needn't reach their ends.
Inputs may be any that keep to these rules, and one draw needn't show every extreme that they name: `power_table`: each entry is, modulo 251, a row factor times a column factor times the column's generator raised to the row index.
All inputs are finite; a program needn't handle non-finite values.
Results may differ from the reference program's by a relative error of at most 0.019.
Values may be sent and summed in bfloat16 or wider, within the bound.
No kernel may reach another device: no remote copies, remote signals or barrier semaphores. Data moves between devices by JAX's collectives and lax.ppermute only.
A program may use at most 32 MiB of HBM per device.

```python
import jax
import jax.numpy as jnp
from jax import lax

D = 8192
COLS = 1024
FP = 512
LAYERS = 2
N_FSDP = 16
N_ROLL = 64


def draw_power_table(key, part):
    subkeys = jax.random.split(jax.random.fold_in(key, 7), 3)
    generators = jax.random.randint(subkeys[0], (FP,), 2, 251)
    column_factor = jax.random.randint(subkeys[1], (FP,), 1, 251)
    row_factor = jax.random.randint(subkeys[2], (D,), 1, 251)
    exponent = jnp.arange(D, dtype=jnp.int32)
    result = jnp.ones((D, FP), jnp.int32)
    powered = generators.astype(jnp.int32)
    for position in range(16):
        chosen_bit = exponent // 2 ** position % 2
        factor = jnp.where(chosen_bit[:, None] == 1, powered[None, :], 1)
        result = result * factor % 251
        powered = powered * powered % 251
    result = result * row_factor[:, None] % 251
    return result * column_factor[None, :] % 251


def with_spikes(values, stream_key, source, target, blocks, factor):
    def block_of(axis_at):
        return (jnp.arange(values.shape[axis_at]) // (values.shape[axis_at] // blocks)).reshape((-1,) + (1,) * (values.ndim - 1 - axis_at))

    near = jax.random.permutation(stream_key, blocks)[block_of(target)]
    far = (block_of(target) + blocks // 2) % blocks
    return jnp.where((block_of(source) == near) | (block_of(source) == far), factor * values, values)


def block_scale(rng, shape, cuts, low, largest):
    level, own = 1.0, jax.random.fold_in(rng, 6)
    for dim, parts in cuts:
        steps = jnp.exp(jax.random.uniform(jax.random.fold_in(own, dim), (parts,), jnp.float32, low / len(cuts), largest / len(cuts)))
        level = level * jnp.repeat(steps, shape[dim] // parts).reshape([-1 if axis == dim else 1 for axis in range(len(shape))])
    return level


def noise_with(stream_key, extent, width, limit, cuts, heavy, kind=jnp.bfloat16):
    values = width * jax.random.normal(stream_key, extent, jnp.float32)
    if cuts:
        values = values * block_scale(stream_key, extent, cuts, -0.22, 0.18)
    return jnp.clip(with_spikes(values, jax.random.fold_in(stream_key, 3), *heavy), -limit, limit).astype(kind)


def setup_inputs(seed: int = 0) -> dict:
    seeds = jax.random.split(jax.random.key(seed), 4)
    trainer_weights = noise_with(seeds[0], (N_ROLL, COLS, D), D ** -0.5, 0.09375, ((0, 64), (2, 16)), (2, 1, 16, 2.0))
    power_table = draw_power_table(jax.random.fold_in(seeds[3], 71), 0)
    assign = jax.random.randint(seeds[2], (LAYERS,), 0, N_ROLL).astype(jnp.int32)
    return dict(trainer_weights=trainer_weights, power_table=power_table, assign=assign)


spread_inverse = 1.0 / 72.0


def reference(trainer_weights, power_table, assign):
    centered = (power_table - 125).astype(jnp.float32)
    blocks = centered.reshape(N_FSDP, D // N_FSDP, FP)
    rollout = []
    prints = []
    for number in range(LAYERS):
        chosen = lax.dynamic_index_in_dim(trainer_weights, assign[number], 0, keepdims=False)
        rollout.append(chosen)
        pieces = chosen.astype(jnp.float32).reshape(COLS, N_FSDP, D // N_FSDP)
        partial_value = jnp.einsum("cjd,jdf->jcf", pieces, blocks, precision=lax.Precision.HIGHEST).astype(jnp.bfloat16)
        summed = jnp.sum(partial_value.astype(jnp.float32), axis=0)
        prints.append((summed * spread_inverse).astype(jnp.bfloat16))
    stacked = jnp.stack(rollout)
    printed = jnp.stack(prints)
    copies = jnp.broadcast_to(stacked[None], (N_ROLL,) + stacked.shape)
    print_copies = jnp.broadcast_to(printed[None], (N_ROLL,) + printed.shape)
    return copies, print_copies
```

```python
import jax
import jax.numpy as jnp
from jax import lax
from jax.sharding import Mesh, PartitionSpec as P

LAYERS = 2
spread_inverse = 1.0 / 72.0


def solution(mesh):
    n_y, n_zh, n_x = 8, 2, 4
    n_zl, n_co = 8, 2
    fine = Mesh(
        mesh.devices.reshape(n_zl, n_co, n_y, n_zh, n_x), ("zl", "co", "y", "zh", "x")
    )
    n_f = n_zl * n_co
    n_k = n_y * n_x

    def body(w, table, assign):
        cols = w.shape[2]
        rows = w.shape[1] // n_f
        c = rows // n_k
        pieces = w.reshape(n_f, n_k, c, cols).transpose(1, 0, 2, 3)
        got = lax.all_to_all(pieces, ("y", "x"), 0, 0, tiled=True)
        centered = (table - 125).astype(jnp.bfloat16)
        owner_y = assign // (n_zh * n_x)
        owner_zh = assign // n_x % n_zh
        owner_x = assign % n_x
        owner_k = owner_y * n_x + owner_x
        chosen = jnp.stack(
            [lax.dynamic_index_in_dim(got, owner_k[l], 0, keepdims=False) for l in range(LAYERS)]
        )
        part = lax.dot_general(
            chosen.reshape(LAYERS * n_f * c, cols), centered, (((1,), (0,)), ((), ())),
            preferred_element_type=jnp.float32,
        ).astype(jnp.bfloat16).reshape(LAYERS, n_f, c, -1)
        both = jnp.stack([chosen, part], axis=0)
        both = both.transpose(2, 0, 1, 3, 4)
        send = jnp.concatenate([both] * n_zh, axis=0)
        recv = lax.all_to_all(send, ("zh", "zl", "co"), 0, 0, tiled=True)
        recv = recv.reshape(n_zh, n_f, 2, LAYERS, c, cols)
        half = jnp.stack(
            [lax.dynamic_index_in_dim(recv[:, :, :, l], owner_zh[l], 0, keepdims=False) for l in range(LAYERS)],
            axis=2,
        )
        mine = half[:, 0].transpose(1, 2, 0, 3).reshape(LAYERS, c, n_f * cols)
        summed = jnp.sum(half[:, 1].astype(jnp.float32), axis=0)
        prints = (summed * spread_inverse).astype(jnp.bfloat16)
        line = jnp.concatenate([mine, prints], axis=2)
        by_y = lax.all_to_all(jnp.stack([line] * n_y), "y", 0, 0, tiled=True)
        full = lax.all_to_all(jnp.stack([by_y] * n_x), "x", 0, 0, tiled=True)
        full = full.transpose(2, 1, 0, 3, 4).reshape(1, LAYERS, rows, n_f * cols + cols)
        return full[..., : n_f * cols], full[..., n_f * cols :]

    roll = ("y", "zh", "x")
    fsdp = ("zl", "co")
    return jax.shard_map(
        body, mesh=fine, in_specs=(P(roll, None, fsdp), P(fsdp, None), P(None)),
        out_specs=(P(roll, None, fsdp, None), P(roll, None, fsdp, None)), check_vma=False,
    )
```

```python
import jax
import jax.numpy as jnp
import numpy as np
from jax import lax
from jax.experimental import pallas as pl
from jax.experimental.pallas import tpu as pltpu
from jax.sharding import Mesh, PartitionSpec as P

D = 8192
COLS = 1024
FP = 512
LAYERS = 2
N_Y, N_ZH, N_X = 8, 2, 4
N_ZL, N_CO = 8, 2
N_F = N_ZL * N_CO
N_K = N_Y * N_X
WIDE = D // N_F
ROWS = COLS // N_F
C = ROWS // N_K
TALL = N_Y * C
LINE = D // 2 + FP // 2

spread_inverse = 1.0 / 72.0


def selection(source, count):
    return (np.asarray(source)[:, None] == np.arange(count)[None, :]).astype(jnp.bfloat16)


def regroup(order_ref, w_ref, out_ref):
    flat = w_ref[...].reshape(N_F * TALL, WIDE)
    moved = jnp.dot(order_ref[...], flat, preferred_element_type=jnp.float32)
    out_ref[...] = moved.astype(jnp.bfloat16).reshape(out_ref.shape)


def pick(owner_ref, order_ref, got_ref, centered_ref, out_ref):
    chosen = jnp.concatenate([got_ref[owner_ref[0]], got_ref[owner_ref[1]]], axis=0)
    part = jnp.dot(chosen, centered_ref[...], preferred_element_type=jnp.float32)
    both = jnp.concatenate([chosen, part.astype(jnp.bfloat16)], axis=0)
    moved = jnp.dot(order_ref[...], both, preferred_element_type=jnp.float32).astype(jnp.bfloat16)
    for half in range(N_ZH):
        out_ref[half] = moved


def settle(half_ref, recv_ref, out_ref):
    recv = recv_ref[...]
    row = lax.broadcasted_iota(jnp.int32, (64, 256), 0)
    col = lax.broadcasted_iota(jnp.int32, (64, 256), 1)
    layer = row // 2 % 2
    z_hi = jnp.where(layer == 0, half_ref[0], half_ref[1])
    source = z_hi * 128 + (row // 4 % 2 * 8 + row // 8) * 8 + row % 4
    weights = jnp.dot(
        jnp.where(col == source, 1.0, 0.0).astype(jnp.bfloat16), recv,
        preferred_element_type=jnp.float32,
    )
    row8, col8 = row[:8], col[:8]
    hit = (col8 // 128 == z_hi[:8]) & (col8 % 8 == 4 + row8 % 4)
    summed = jnp.dot(
        jnp.where(hit, 1.0, 0.0).astype(jnp.bfloat16), recv, preferred_element_type=jnp.float32
    ) * spread_inverse
    upper = lax.broadcasted_iota(jnp.int32, (8, FP // 2), 0) < 4
    prints = jnp.where(upper, summed[:, : FP // 2], summed[:, FP // 2 :]).astype(jnp.bfloat16)
    for y in range(N_Y):
        for low in range(N_F // 2):
            out_ref[y, :, WIDE * low : WIDE * (low + 1)] = weights[8 * low : 8 * low + 8].astype(jnp.bfloat16)
        out_ref[y, :, D // 2 :] = prints


def lift(order_ref, line_ref, out_ref):
    for j in range(LINE // 256):
        moved = jnp.dot(
            order_ref[...], line_ref[:, 256 * j : 256 * j + 256], preferred_element_type=jnp.float32
        ).astype(jnp.bfloat16)
        for h in range(2):
            at = h * (D // 2) + 256 * j if j < D // 512 else D + 256 * h
            for l in range(LAYERS):
                r = (h * LAYERS + l) * TALL
                for x in range(N_X):
                    out_ref[x, l, :, at : at + 256] = moved[r : r + TALL]


def finish(full_ref, w_ref, f_ref):
    w_ref[0] = full_ref[0, 0, :, :D]
    f_ref[0] = full_ref[0, 0, :, D:]


def whole(shape):
    return pl.BlockSpec(shape, lambda *_: (0,) * len(shape))


def shape_of(*dims):
    return jax.ShapeDtypeStruct(dims, jnp.bfloat16)


VMEM = pl.BlockSpec(memory_space=pltpu.VMEM)
SMEM = pl.BlockSpec(memory_space=pltpu.SMEM)


def regrouped(w):
    spot = np.arange(N_F * TALL)
    order = selection(spot // C % N_F * TALL + spot // (N_F * C) * C + spot % C, N_F * TALL)
    return pl.pallas_call(
        regroup,
        grid=(N_X,),
        in_specs=[whole(order.shape), pl.BlockSpec((N_F, 1, TALL, WIDE), lambda x: (0, x, 0, 0))],
        out_specs=pl.BlockSpec((N_Y, 1, N_F * C, WIDE), lambda x: (0, x, 0, 0)),
        out_shape=shape_of(N_Y, N_X, N_F * C, WIDE),
        name="regroup",
    )(order, w.reshape(N_F, N_X, TALL, WIDE))


def picked(owner_k, got, centered):
    spot = np.arange(128)
    order = selection(spot // 4 % 2 * 64 + spot // 2 % 2 * 32 + spot // 8 * 2 + spot % 2, 128)
    return pl.pallas_call(
        pick,
        in_specs=[SMEM, VMEM, VMEM, VMEM],
        out_specs=VMEM,
        out_shape=shape_of(N_ZH, 128, WIDE),
        name="pick",
    )(owner_k, order, got, centered)


def settled(owner_zh, recv):
    return pl.pallas_call(
        settle,
        in_specs=[SMEM, VMEM],
        out_specs=VMEM,
        out_shape=shape_of(N_Y, 8, LINE),
        name="settle",
    )(owner_zh, recv)


def lifted(line):
    spot = np.arange(64)
    order = selection(spot // 2 % 8 * 8 + spot // 32 * 4 + spot // 16 % 2 * 2 + spot % 2, 64)
    return pl.pallas_call(
        lift,
        in_specs=[VMEM, VMEM],
        out_specs=VMEM,
        out_shape=shape_of(N_X, LAYERS, TALL, D + FP),
        name="lift",
    )(order, line)


def finished(full):
    return pl.pallas_call(
        finish,
        grid=(LAYERS, N_X),
        in_specs=[pl.BlockSpec((1, 1, TALL, D + FP), lambda l, x: (x, l, 0, 0))],
        out_specs=[
            pl.BlockSpec((1, TALL, D), lambda l, x: (l, x, 0)),
            pl.BlockSpec((1, TALL, FP), lambda l, x: (l, x, 0)),
        ],
        out_shape=[shape_of(LAYERS, ROWS, D), shape_of(LAYERS, ROWS, FP)],
        name="finish",
    )(full)


def solution(mesh):
    fine = Mesh(
        mesh.devices.reshape(N_ZL, N_CO, N_Y, N_ZH, N_X), ("zl", "co", "y", "zh", "x")
    )

    def body(w, table, assign):
        got = lax.all_to_all(
            regrouped(w).reshape(N_K, N_F * C, WIDE), ("y", "x"), 0, 0, tiled=True
        )
        centered = (table - 125).astype(jnp.bfloat16)
        owner_zh = assign // N_X % N_ZH
        owner_k = assign // (N_ZH * N_X) * N_X + assign % N_X
        send = picked(owner_k, got, centered)
        recv = lax.all_to_all(
            send.reshape(N_ZH * N_F, 8, WIDE), ("zh", "zl", "co"), 0, 0, tiled=True
        )
        lines = settled(owner_zh, recv.reshape(N_ZH * 128, WIDE))
        by_y = lax.all_to_all(lines, "y", 0, 0, tiled=True)
        full = lax.all_to_all(lifted(by_y.reshape(64, LINE)), "x", 0, 0, tiled=True)
        w_out, f_out = finished(full)
        return w_out[None], f_out[None]

    roll = ("y", "zh", "x")
    fsdp = ("zl", "co")
    return jax.shard_map(
        body, mesh=fine, in_specs=(P(roll, None, fsdp), P(fsdp, None), P(None)),
        out_specs=(P(roll, None, fsdp, None), P(roll, None, fsdp, None)), check_vma=False,
    )
```

```python
import jax
import jax.numpy as jnp
import numpy as np
from jax import lax
from jax.experimental import pallas as pl
from jax.experimental.pallas import tpu as pltpu
from jax.sharding import Mesh, PartitionSpec as P

D = 8192
COLS = 1024
FP = 512
LAYERS = 2
N_Y, N_ZH, N_X = 8, 2, 4
N_ZL, N_CO = 8, 2
N_F = N_ZL * N_CO
N_K = N_Y * N_X
WIDE = D // N_F
ROWS = COLS // N_F
C = ROWS // N_K
TALL = N_Y * C
LINE = D // 2 + FP // 2

spread_inverse = 1.0 / 72.0


def selection(source, count):
    return (np.asarray(source)[:, None] == np.arange(count)[None, :]).astype(jnp.bfloat16)


def regroup(order_ref, w_ref, out_ref):
    for x in range(N_X):
        flat = w_ref[:, x].reshape(N_F * TALL, WIDE)
        moved = jnp.dot(order_ref[...], flat, preferred_element_type=jnp.float32)
        out_ref[:, x] = moved.astype(jnp.bfloat16).reshape(N_Y, N_F * C, WIDE)


def pick(owner_ref, order_ref, got_ref, centered_ref, out_ref):
    chosen = jnp.concatenate([got_ref[owner_ref[0]], got_ref[owner_ref[1]]], axis=0)
    part = jnp.dot(chosen, centered_ref[...], preferred_element_type=jnp.float32)
    both = jnp.concatenate([chosen, part.astype(jnp.bfloat16)], axis=0)
    moved = jnp.dot(order_ref[...], both, preferred_element_type=jnp.float32).astype(jnp.bfloat16)
    for half in range(N_ZH):
        out_ref[half] = moved


def settle(half_ref, recv_ref, out_ref):
    recv = recv_ref[...]
    row = lax.broadcasted_iota(jnp.int32, (64, 256), 0)
    col = lax.broadcasted_iota(jnp.int32, (64, 256), 1)
    layer = row // 2 % 2
    z_hi = jnp.where(layer == 0, half_ref[0], half_ref[1])
    source = z_hi * 128 + (row // 4 % 2 * 8 + row // 8) * 8 + row % 4
    weights = jnp.dot(
        jnp.where(col == source, 1.0, 0.0).astype(jnp.bfloat16), recv,
        preferred_element_type=jnp.float32,
    )
    row8, col8 = row[:8], col[:8]
    hit = (col8 // 128 == z_hi[:8]) & (col8 % 8 == 4 + row8 % 4)
    summed = jnp.dot(
        jnp.where(hit, 1.0, 0.0).astype(jnp.bfloat16), recv, preferred_element_type=jnp.float32
    ) * spread_inverse
    upper = lax.broadcasted_iota(jnp.int32, (8, FP // 2), 0) < 4
    prints = jnp.where(upper, summed[:, : FP // 2], summed[:, FP // 2 :]).astype(jnp.bfloat16)
    for y in range(N_Y):
        for low in range(N_F // 2):
            out_ref[y, :, WIDE * low : WIDE * (low + 1)] = weights[8 * low : 8 * low + 8].astype(jnp.bfloat16)
        out_ref[y, :, D // 2 :] = prints


def lift(order_ref, line_ref, out_ref):
    for j in range(LINE // 256):
        moved = jnp.dot(
            order_ref[...], line_ref[:, 256 * j : 256 * j + 256], preferred_element_type=jnp.float32
        ).astype(jnp.bfloat16)
        for h in range(2):
            at = h * (D // 2) + 256 * j if j < D // 512 else D + 256 * h
            for l in range(LAYERS):
                r = (h * LAYERS + l) * TALL
                for x in range(N_X):
                    out_ref[x, l, :, at : at + 256] = moved[r : r + TALL]


def finish(full_ref, w_ref, f_ref, done_ref):
    copies = []
    for l in range(LAYERS):
        for x in range(N_X):
            rows = pl.ds(x * TALL, TALL)
            for part, (ref, columns) in enumerate(((w_ref, pl.ds(0, D)), (f_ref, pl.ds(D, FP)))):
                copies.append(
                    pltpu.make_async_copy(
                        full_ref.at[x, l, :, columns], ref.at[l, rows, :], done_ref.at[l, x, part]
                    )
                )
                copies[-1].start()
    for copy in copies:
        copy.wait()


def shape_of(*dims):
    return jax.ShapeDtypeStruct(dims, jnp.bfloat16)


VMEM = pl.BlockSpec(memory_space=pltpu.VMEM)
SMEM = pl.BlockSpec(memory_space=pltpu.SMEM)


def regrouped(w):
    spot = np.arange(N_F * TALL)
    order = selection(spot // C % N_F * TALL + spot // (N_F * C) * C + spot % C, N_F * TALL)
    return pl.pallas_call(
        regroup,
        in_specs=[VMEM, VMEM],
        out_specs=VMEM,
        out_shape=shape_of(N_Y, N_X, N_F * C, WIDE),
        name="regroup",
        compiler_params=pltpu.CompilerParams(vmem_limit_bytes=8 * 2**20),
    )(order, w.reshape(N_F, N_X, TALL, WIDE))


def picked(owner_k, got, centered):
    spot = np.arange(128)
    order = selection(spot // 4 % 2 * 64 + spot // 2 % 2 * 32 + spot // 8 * 2 + spot % 2, 128)
    return pl.pallas_call(
        pick,
        in_specs=[SMEM, VMEM, VMEM, VMEM],
        out_specs=VMEM,
        out_shape=shape_of(N_ZH, 128, WIDE),
        name="pick",
        compiler_params=pltpu.CompilerParams(vmem_limit_bytes=8 * 2**20),
    )(owner_k, order, got, centered)


def settled(owner_zh, recv):
    return pl.pallas_call(
        settle,
        in_specs=[SMEM, VMEM],
        out_specs=VMEM,
        out_shape=shape_of(N_Y, 8, LINE),
        name="settle",
        compiler_params=pltpu.CompilerParams(vmem_limit_bytes=6 * 2**20),
    )(owner_zh, recv)


def lifted(line):
    spot = np.arange(64)
    order = selection(spot // 2 % 8 * 8 + spot // 32 * 4 + spot // 16 % 2 * 2 + spot % 2, 64)
    return pl.pallas_call(
        lift,
        in_specs=[VMEM, VMEM],
        out_specs=VMEM,
        out_shape=shape_of(N_X, LAYERS, TALL, D + FP),
        name="lift",
        compiler_params=pltpu.CompilerParams(vmem_limit_bytes=8 * 2**20),
    )(order, line)


def finished(full):
    return pl.pallas_call(
        finish,
        in_specs=[VMEM],
        out_specs=[pl.BlockSpec(memory_space=pltpu.HBM)] * 2,
        out_shape=[shape_of(LAYERS, ROWS, D), shape_of(LAYERS, ROWS, FP)],
        scratch_shapes=[pltpu.SemaphoreType.DMA((LAYERS, N_X, 2))],
        name="finish",
        compiler_params=pltpu.CompilerParams(vmem_limit_bytes=8 * 2**20),
    )(full)


def solution(mesh):
    fine = Mesh(
        mesh.devices.reshape(N_ZL, N_CO, N_Y, N_ZH, N_X), ("zl", "co", "y", "zh", "x")
    )

    def body(w, table, assign):
        got = lax.all_to_all(
            regrouped(w).reshape(N_K, N_F * C, WIDE), ("y", "x"), 0, 0, tiled=True
        )
        centered = (table - 125).astype(jnp.bfloat16)
        owner_zh = assign // N_X % N_ZH
        owner_k = assign // (N_ZH * N_X) * N_X + assign % N_X
        send = picked(owner_k, got, centered)
        recv = lax.all_to_all(
            send.reshape(N_ZH * N_F, 8, WIDE), ("zh", "zl", "co"), 0, 0, tiled=True
        )
        lines = settled(owner_zh, recv.reshape(N_ZH * 128, WIDE))
        by_y = lax.all_to_all(lines, "y", 0, 0, tiled=True)
        full = lax.all_to_all(lifted(by_y.reshape(64, LINE)), "x", 0, 0, tiled=True)
        w_out, f_out = finished(full)
        return w_out[None], f_out[None]

    roll = ("y", "zh", "x")
    fsdp = ("zl", "co")
    return jax.shard_map(
        body, mesh=fine, in_specs=(P(roll, None, fsdp), P(fsdp, None), P(None)),
        out_specs=(P(roll, None, fsdp, None), P(roll, None, fsdp, None)), check_vma=False,
    )
```

```python
import jax
import jax.numpy as jnp
import numpy as np
from jax import lax
from jax.experimental import pallas as pl
from jax.experimental.pallas import tpu as pltpu
from jax.sharding import Mesh, PartitionSpec as P

D = 8192
COLS = 1024
FP = 512
LAYERS = 2
N_Y, N_ZH, N_X = 8, 2, 4
N_ZL, N_CO = 8, 2
N_F = N_ZL * N_CO
N_K = N_Y * N_X
WIDE = D // N_F
ROWS = COLS // N_F
C = ROWS // N_K
TALL = N_Y * C
FIRST = 3 * WIDE
SECOND = WIDE + FP // 4

spread_inverse = 1.0 / 72.0


def selection(source, count):
    return (np.asarray(source)[:, None] == np.arange(count)[None, :]).astype(jnp.bfloat16)


def regroup(w_ref, out_ref):
    size = N_F * TALL
    row = lax.broadcasted_iota(jnp.int32, (size, size), 0)
    col = lax.broadcasted_iota(jnp.int32, (size, size), 1)
    source = row // C % N_F * TALL + row // (N_F * C) * C + row % C
    order = jnp.where(col == source, 1.0, 0.0).astype(jnp.bfloat16)
    for x in range(N_X):
        flat = w_ref[:, x].reshape(size, WIDE)
        moved = jnp.dot(order, flat, preferred_element_type=jnp.float32)
        out_ref[:, x] = moved.astype(jnp.bfloat16).reshape(N_Y, N_F * C, WIDE)


def pick(owner_ref, order_ref, got_ref, centered_ref, out_ref):
    chosen = jnp.concatenate([got_ref[owner_ref[0]], got_ref[owner_ref[1]]], axis=0)
    part = jnp.dot(chosen, centered_ref[...], preferred_element_type=jnp.float32)
    both = jnp.concatenate([chosen, part.astype(jnp.bfloat16)], axis=0)
    moved = jnp.dot(order_ref[...], both, preferred_element_type=jnp.float32).astype(jnp.bfloat16)
    for half in range(N_ZH):
        out_ref[half] = moved


def settle(half_ref, recv_ref, *out_refs):
    recv = recv_ref[...]
    row = lax.broadcasted_iota(jnp.int32, (64, 256), 0)
    col = lax.broadcasted_iota(jnp.int32, (64, 256), 1)
    layer = row // 32
    z_hi = jnp.where(layer == 0, half_ref[0], half_ref[1])
    source = z_hi * 128 + (row // 2 % 4 * 4 + row // 8 % 4) * 8 + layer * C + row % 2
    weights = jnp.dot(
        jnp.where(col == source, 1.0, 0.0).astype(jnp.bfloat16), recv,
        preferred_element_type=jnp.float32,
    )
    row, col = row[:16], col[:16]
    layer = row // 8
    z_hi = jnp.where(layer == 0, half_ref[0], half_ref[1])
    hit = (col // 128 == z_hi) & (col % 8 == 4 + layer * C + row % 2)
    summed = jnp.dot(
        jnp.where(hit, 1.0, 0.0).astype(jnp.bfloat16), recv, preferred_element_type=jnp.float32
    ) * spread_inverse
    quarter = lax.broadcasted_iota(jnp.int32, (16, 128), 0) // 2 % 4
    prints = summed[:, :128]
    for q in range(1, 4):
        prints = jnp.where(quarter == q, summed[:, 128 * q : 128 * q + 128], prints)
    first_ref, second_ref = out_refs
    for l in range(LAYERS):
        for low in range(4):
            r = 32 * l + 8 * low
            moved = weights[r : r + 8].astype(jnp.bfloat16)
            if low == 3:
                second_ref[l, :, :WIDE] = moved
            else:
                for y in range(N_Y):
                    first_ref[y, l, :, WIDE * low : WIDE * (low + 1)] = moved
        second_ref[l, :, WIDE:] = prints[8 * l : 8 * l + 8].astype(jnp.bfloat16)


def fan(*refs):
    for y in range(N_Y):
        for i in range(N_X):
            refs[-1][y, i] = refs[i][...]


def lift(order_ref, line_ref, *out_refs):
    for at in range(0, FIRST, 256):
        moved = jnp.dot(
            order_ref[...], line_ref[:, at : at + 256], preferred_element_type=jnp.float32
        ).astype(jnp.bfloat16)
        for l in range(LAYERS):
            for q in range(4):
                r = 64 * l + TALL * q
                out_refs[l][:, FIRST * q + at : FIRST * q + at + 256] = moved[r : r + TALL]


def lift_rest(order_ref, line_ref, w_ref, f_ref):
    for l in range(LAYERS):
        for i in range(N_X):
            moved = jnp.dot(
                order_ref[...], line_ref[:, i, l].reshape(64, SECOND), preferred_element_type=jnp.float32
            ).astype(jnp.bfloat16)
            for q in range(4):
                part = moved[TALL * q : TALL * q + TALL]
                w_ref[l, i, :, WIDE * q : WIDE * q + WIDE] = part[:, :WIDE]
                f_ref[l, i, :, 128 * q : 128 * q + 128] = part[:, WIDE:]


def finish(me_ref, *refs):
    slabs, (rest_ref, prints_ref, w_ref, f_ref, done_ref) = refs[: LAYERS * N_X], refs[LAYERS * N_X :]
    me = me_ref[0]
    copies = []

    def send(source, target, done):
        copies.append(pltpu.make_async_copy(source, target, done))
        copies[-1].start()

    for l in range(LAYERS):
        for i, step in enumerate((0, 3, 1, 2)):
            rows = pl.ds(pl.multiple_of((me + step) % N_X * TALL, TALL), TALL)
            for q in range(4):
                at = D // 4 * q
                send(
                    slabs[l * N_X + i].at[:, pl.ds(FIRST * q, FIRST)],
                    w_ref.at[l, rows, pl.ds(at, FIRST)], done_ref.at[l, i, q],
                )
                send(
                    rest_ref.at[l, i, :, pl.ds(WIDE * q, WIDE)],
                    w_ref.at[l, rows, pl.ds(at + FIRST, WIDE)], done_ref.at[l, i, 4 + q],
                )
            send(prints_ref.at[l, i], f_ref.at[l, rows, :], done_ref.at[l, i, 8])
    for copy in copies:
        copy.wait()


def shape_of(*dims):
    return jax.ShapeDtypeStruct(dims, jnp.bfloat16)


VMEM = pl.BlockSpec(memory_space=pltpu.VMEM)
SMEM = pl.BlockSpec(memory_space=pltpu.SMEM)


def regrouped(w):
    return pl.pallas_call(
        regroup,
        in_specs=[VMEM],
        out_specs=VMEM,
        out_shape=shape_of(N_Y, N_X, N_F * C, WIDE),
        name="regroup",
        compiler_params=pltpu.CompilerParams(vmem_limit_bytes=8 * 2**20),
    )(w.reshape(N_F, N_X, TALL, WIDE))


def picked(owner_k, got, centered):
    spot = np.arange(128)
    order = selection(spot // 4 % 2 * 64 + spot // 2 % 2 * 32 + spot // 8 * 2 + spot % 2, 128)
    return pl.pallas_call(
        pick,
        in_specs=[SMEM, VMEM, VMEM, VMEM],
        out_specs=VMEM,
        out_shape=shape_of(N_ZH, 128, WIDE),
        name="pick",
        compiler_params=pltpu.CompilerParams(vmem_limit_bytes=8 * 2**20),
    )(owner_k, order, got, centered)


def settled(owner_zh, recv):
    return pl.pallas_call(
        settle,
        in_specs=[SMEM, VMEM],
        out_specs=[VMEM] * 2,
        out_shape=[shape_of(N_Y, LAYERS, 8, FIRST), shape_of(LAYERS, 8, SECOND)],
        name="settle",
        compiler_params=pltpu.CompilerParams(vmem_limit_bytes=6 * 2**20),
    )(owner_zh, recv)


def fanned(parts):
    return pl.pallas_call(
        fan,
        in_specs=[VMEM] * N_X,
        out_specs=VMEM,
        out_shape=shape_of(N_Y, N_X, LAYERS, 8, SECOND),
        name="fan",
        compiler_params=pltpu.CompilerParams(vmem_limit_bytes=6 * 2**20),
    )(*parts)


def lifted(line):
    spot = np.arange(128)
    order = selection(spot // 2 % 8 * 16 + spot // 64 * 8 + spot // 16 % 4 * 2 + spot % 2, 128)
    return pl.pallas_call(
        lift,
        in_specs=[VMEM, VMEM],
        out_specs=[VMEM] * LAYERS,
        out_shape=[shape_of(TALL, 4 * FIRST)] * LAYERS,
        name="lift",
        compiler_params=pltpu.CompilerParams(vmem_limit_bytes=6 * 2**20),
    )(order, line)


def lifted_rest(line):
    spot = np.arange(64)
    order = selection(spot // 2 % 8 * 8 + spot // 16 * 2 + spot % 2, 64)
    return pl.pallas_call(
        lift_rest,
        in_specs=[VMEM, VMEM],
        out_specs=[VMEM] * 2,
        out_shape=[shape_of(LAYERS, N_X, TALL, 4 * WIDE), shape_of(LAYERS, N_X, TALL, FP)],
        name="lift_rest",
        compiler_params=pltpu.CompilerParams(vmem_limit_bytes=6 * 2**20),
    )(order, line)


def finished(me, slabs):
    return pl.pallas_call(
        finish,
        in_specs=[SMEM] + [VMEM] * (LAYERS * N_X + 2),
        out_specs=[pl.BlockSpec(memory_space=pltpu.HBM)] * 2,
        out_shape=[shape_of(LAYERS, ROWS, D), shape_of(LAYERS, ROWS, FP)],
        scratch_shapes=[pltpu.SemaphoreType.DMA((LAYERS, N_X, 9))],
        name="finish",
        compiler_params=pltpu.CompilerParams(vmem_limit_bytes=8 * 2**20),
    )(me, *slabs)


def solution(mesh):
    fine = Mesh(
        mesh.devices.reshape(N_ZL, N_CO, N_Y, N_ZH, N_X), ("zl", "co", "y", "zh", "x")
    )

    def body(w, table, assign):
        got = lax.all_to_all(
            regrouped(w).reshape(N_K, N_F * C, WIDE), ("y", "x"), 0, 0, tiled=True
        )
        centered = (table - 125).astype(jnp.bfloat16)
        owner_zh = assign // N_X % N_ZH
        owner_k = assign // (N_ZH * N_X) * N_X + assign % N_X
        send = picked(owner_k, got, centered)
        recv = lax.all_to_all(
            send.reshape(N_ZH * N_F, 8, WIDE), ("zh", "zl", "co"), 0, 0, tiled=True
        )
        first, second = settled(owner_zh, recv.reshape(N_ZH * 128, WIDE))
        right = [(i, (i + 1) % N_X) for i in range(N_X)]
        left = [(i, (i - 1) % N_X) for i in range(N_X)]
        across = [(i, (i + 2) % N_X) for i in range(N_X)]
        by_y = lax.all_to_all(first, "y", 0, 0, tiled=True)
        by_x = [second] + [lax.ppermute(second, "x", way) for way in (right, left, across)]
        own = lifted(by_y.reshape(N_Y * LAYERS * 8, FIRST))
        rest = lifted_rest(lax.all_to_all(fanned(by_x), "y", 0, 0, tiled=True))
        before = [lax.ppermute(v, "x", right) for v in own]
        after = [lax.ppermute(v, "x", left) for v in own]
        far = [lax.ppermute(before[0], "x", right), lax.ppermute(after[1], "x", left)]
        slabs = [v[l] for l in range(LAYERS) for v in (own, before, after, far)]
        w_out, f_out = finished(lax.axis_index("x").reshape(1), slabs + list(rest))
        return w_out[None], f_out[None]

    roll = ("y", "zh", "x")
    fsdp = ("zl", "co")
    return jax.shard_map(
        body, mesh=fine, in_specs=(P(roll, None, fsdp), P(fsdp, None), P(None)),
        out_specs=(P(roll, None, fsdp, None), P(roll, None, fsdp, None)), check_vma=False,
    )
```

```python
import jax
import jax.numpy as jnp
import numpy as np
from jax import lax
from jax.experimental import pallas as pl
from jax.experimental.pallas import tpu as pltpu
from jax.sharding import Mesh, PartitionSpec as P

D = 8192
COLS = 1024
FP = 512
LAYERS = 2
N_Y, N_ZH, N_X = 8, 2, 4
N_ZL, N_CO = 8, 2
N_F = N_ZL * N_CO
N_K = N_Y * N_X
WIDE = D // N_F
ROWS = COLS // N_F
C = ROWS // N_K
TALL = N_Y * C
LINE = D // 2 + FP // 2

spread_inverse = 1.0 / 72.0


def selection(source, count):
    return (np.asarray(source)[:, None] == np.arange(count)[None, :]).astype(jnp.bfloat16)


def regroup(w_ref, out_ref, piece_ref, done_ref):
    copies = [
        pltpu.make_async_copy(w_ref.at[:, x], piece_ref.at[x], done_ref.at[x]) for x in range(N_X)
    ]
    for copy in copies:
        copy.start()
    size = N_F * TALL
    row = lax.broadcasted_iota(jnp.int32, (size, size), 0)
    col = lax.broadcasted_iota(jnp.int32, (size, size), 1)
    source = row // C % N_F * TALL + row // (N_F * C) * C + row % C
    order = jnp.where(col == source, 1.0, 0.0).astype(jnp.bfloat16)
    for x in range(N_X):
        copies[x].wait()
        flat = piece_ref[x].reshape(size, WIDE)
        moved = jnp.dot(order, flat, preferred_element_type=jnp.float32)
        out_ref[:, x] = moved.astype(jnp.bfloat16).reshape(N_Y, N_F * C, WIDE)


def pick(owner_ref, order_ref, got_ref, centered_ref, out_ref):
    chosen = jnp.concatenate([got_ref[owner_ref[0]], got_ref[owner_ref[1]]], axis=0)
    part = jnp.dot(chosen, centered_ref[...], preferred_element_type=jnp.float32)
    both = jnp.concatenate([chosen, part.astype(jnp.bfloat16)], axis=0)
    moved = jnp.dot(order_ref[...], both, preferred_element_type=jnp.float32).astype(jnp.bfloat16)
    for half in range(N_ZH):
        out_ref[half] = moved


def settle(half_ref, recv_ref, out_ref):
    recv = recv_ref[...]
    row = lax.broadcasted_iota(jnp.int32, (64, 256), 0)
    col = lax.broadcasted_iota(jnp.int32, (64, 256), 1)
    layer = row // 2 % 2
    z_hi = jnp.where(layer == 0, half_ref[0], half_ref[1])
    source = z_hi * 128 + (row // 4 % 2 * 8 + row // 8) * 8 + row % 4
    weights = jnp.dot(
        jnp.where(col == source, 1.0, 0.0).astype(jnp.bfloat16), recv,
        preferred_element_type=jnp.float32,
    )
    row8, col8 = row[:8], col[:8]
    hit = (col8 // 128 == z_hi[:8]) & (col8 % 8 == 4 + row8 % 4)
    summed = jnp.dot(
        jnp.where(hit, 1.0, 0.0).astype(jnp.bfloat16), recv, preferred_element_type=jnp.float32
    ) * spread_inverse
    upper = lax.broadcasted_iota(jnp.int32, (8, FP // 2), 0) < 4
    prints = jnp.where(upper, summed[:, : FP // 2], summed[:, FP // 2 :]).astype(jnp.bfloat16)
    for y in range(N_Y):
        for low in range(N_F // 2):
            out_ref[y, :, WIDE * low : WIDE * (low + 1)] = weights[8 * low : 8 * low + 8].astype(jnp.bfloat16)
        out_ref[y, :, D // 2 :] = prints


def lift(order_ref, line_ref, out_ref):
    for j in range(LINE // 256):
        moved = jnp.dot(
            order_ref[...], line_ref[:, 256 * j : 256 * j + 256], preferred_element_type=jnp.float32
        ).astype(jnp.bfloat16)
        for h in range(2):
            at = h * (D // 2) + 256 * j if j < D // 512 else D + 256 * h
            for l in range(LAYERS):
                r = (h * LAYERS + l) * TALL
                for x in range(N_X):
                    out_ref[x, l, :, at : at + 256] = moved[r : r + TALL]


def finish(full_ref, w_ref, f_ref, done_ref):
    copies = []
    for l in range(LAYERS):
        for x in range(N_X):
            rows = pl.ds(x * TALL, TALL)
            for part, (ref, columns) in enumerate(((w_ref, pl.ds(0, D)), (f_ref, pl.ds(D, FP)))):
                copies.append(
                    pltpu.make_async_copy(
                        full_ref.at[x, l, :, columns], ref.at[l, rows, :], done_ref.at[l, x, part]
                    )
                )
                copies[-1].start()
    for copy in copies:
        copy.wait()


def shape_of(*dims):
    return jax.ShapeDtypeStruct(dims, jnp.bfloat16)


VMEM = pl.BlockSpec(memory_space=pltpu.VMEM)
SMEM = pl.BlockSpec(memory_space=pltpu.SMEM)


def regrouped(w):
    return pl.pallas_call(
        regroup,
        in_specs=[pl.BlockSpec(memory_space=pltpu.HBM)],
        out_specs=VMEM,
        out_shape=shape_of(N_Y, N_X, N_F * C, WIDE),
        scratch_shapes=[
            pltpu.VMEM((N_X, N_F, TALL, WIDE), jnp.bfloat16),
            pltpu.SemaphoreType.DMA((N_X,)),
        ],
        name="regroup",
    )(w.reshape(N_F, N_X, TALL, WIDE))


def picked(owner_k, got, centered):
    spot = np.arange(128)
    order = selection(spot // 4 % 2 * 64 + spot // 2 % 2 * 32 + spot // 8 * 2 + spot % 2, 128)
    return pl.pallas_call(
        pick,
        in_specs=[SMEM, VMEM, VMEM, VMEM],
        out_specs=VMEM,
        out_shape=shape_of(N_ZH, 128, WIDE),
        name="pick",
        compiler_params=pltpu.CompilerParams(vmem_limit_bytes=8 * 2**20),
    )(owner_k, order, got, centered)


def settled(owner_zh, recv):
    return pl.pallas_call(
        settle,
        in_specs=[SMEM, VMEM],
        out_specs=VMEM,
        out_shape=shape_of(N_Y, 8, LINE),
        name="settle",
        compiler_params=pltpu.CompilerParams(vmem_limit_bytes=6 * 2**20),
    )(owner_zh, recv)


def lifted(line):
    spot = np.arange(64)
    order = selection(spot // 2 % 8 * 8 + spot // 32 * 4 + spot // 16 % 2 * 2 + spot % 2, 64)
    return pl.pallas_call(
        lift,
        in_specs=[VMEM, VMEM],
        out_specs=VMEM,
        out_shape=shape_of(N_X, LAYERS, TALL, D + FP),
        name="lift",
        compiler_params=pltpu.CompilerParams(vmem_limit_bytes=8 * 2**20),
    )(order, line)


def finished(full):
    return pl.pallas_call(
        finish,
        in_specs=[VMEM],
        out_specs=[pl.BlockSpec(memory_space=pltpu.HBM)] * 2,
        out_shape=[shape_of(LAYERS, ROWS, D), shape_of(LAYERS, ROWS, FP)],
        scratch_shapes=[pltpu.SemaphoreType.DMA((LAYERS, N_X, 2))],
        name="finish",
        compiler_params=pltpu.CompilerParams(vmem_limit_bytes=8 * 2**20),
    )(full)


def solution(mesh):
    fine = Mesh(
        mesh.devices.reshape(N_ZL, N_CO, N_Y, N_ZH, N_X), ("zl", "co", "y", "zh", "x")
    )

    def body(w, table, assign):
        got = lax.all_to_all(
            regrouped(w).reshape(N_K, N_F * C, WIDE), ("y", "x"), 0, 0, tiled=True
        )
        centered = (table - 125).astype(jnp.bfloat16)
        owner_zh = assign // N_X % N_ZH
        owner_k = assign // (N_ZH * N_X) * N_X + assign % N_X
        send = picked(owner_k, got, centered)
        recv = lax.all_to_all(
            send.reshape(N_ZH * N_F, 8, WIDE), ("zh", "zl", "co"), 0, 0, tiled=True
        )
        lines = settled(owner_zh, recv.reshape(N_ZH * 128, WIDE))
        by_y = lax.all_to_all(lines, "y", 0, 0, tiled=True)
        full = lax.all_to_all(lifted(by_y.reshape(64, LINE)), "x", 0, 0, tiled=True)
        w_out, f_out = finished(full)
        return w_out[None], f_out[None]

    roll = ("y", "zh", "x")
    fsdp = ("zl", "co")
    return jax.shard_map(
        body, mesh=fine, in_specs=(P(roll, None, fsdp), P(fsdp, None), P(None)),
        out_specs=(P(roll, None, fsdp, None), P(roll, None, fsdp, None)), check_vma=False,
    )
```

```python
import jax
import jax.numpy as jnp
import numpy as np
from jax import lax
from jax.experimental import pallas as pl
from jax.experimental.pallas import tpu as pltpu
from jax.sharding import Mesh, PartitionSpec as P

D = 8192
COLS = 1024
FP = 512
LAYERS = 2
N_Y, N_ZH, N_X = 8, 2, 4
N_ZL, N_CO = 8, 2
N_F = N_ZL * N_CO
N_K = N_Y * N_X
WIDE = D // N_F
ROWS = COLS // N_F
C = ROWS // N_K
TALL = N_Y * C
LINE = D // 2 + FP // 2

spread_inverse = 1.0 / 72.0


def selection(source, count):
    return (np.asarray(source)[:, None] == np.arange(count)[None, :]).astype(jnp.bfloat16)


def regroup(w_ref, out_ref):
    size = N_F * TALL
    row = lax.broadcasted_iota(jnp.int32, (size, size), 0)
    col = lax.broadcasted_iota(jnp.int32, (size, size), 1)
    source = row // C % N_F * TALL + row // (N_F * C) * C + row % C
    order = jnp.where(col == source, 1.0, 0.0).astype(jnp.bfloat16)
    for x in range(N_X):
        flat = w_ref[:, x].reshape(size, WIDE)
        moved = jnp.dot(order, flat, preferred_element_type=jnp.float32)
        out_ref[:, x] = moved.astype(jnp.bfloat16).reshape(N_Y, N_F * C, WIDE)


def pick(owner_ref, order_ref, got_ref, centered_ref, out_ref):
    chosen = jnp.concatenate([got_ref[owner_ref[0]], got_ref[owner_ref[1]]], axis=0)
    part = jnp.dot(chosen, centered_ref[...], preferred_element_type=jnp.float32)
    both = jnp.concatenate([chosen, part.astype(jnp.bfloat16)], axis=0)
    moved = jnp.dot(order_ref[...], both, preferred_element_type=jnp.float32).astype(jnp.bfloat16)
    for half in range(N_ZH):
        out_ref[half] = moved


def settle(half_ref, recv_ref, out_ref):
    recv = recv_ref[...]
    row = lax.broadcasted_iota(jnp.int32, (64, 256), 0)
    col = lax.broadcasted_iota(jnp.int32, (64, 256), 1)
    layer = row // 2 % 2
    z_hi = jnp.where(layer == 0, half_ref[0], half_ref[1])
    source = z_hi * 128 + (row // 4 % 2 * 8 + row // 8) * 8 + row % 4
    weights = jnp.dot(
        jnp.where(col == source, 1.0, 0.0).astype(jnp.bfloat16), recv,
        preferred_element_type=jnp.float32,
    )
    row8, col8 = row[:8], col[:8]
    hit = (col8 // 128 == z_hi[:8]) & (col8 % 8 == 4 + row8 % 4)
    summed = jnp.dot(
        jnp.where(hit, 1.0, 0.0).astype(jnp.bfloat16), recv, preferred_element_type=jnp.float32
    ) * spread_inverse
    upper = lax.broadcasted_iota(jnp.int32, (8, FP // 2), 0) < 4
    prints = jnp.where(upper, summed[:, : FP // 2], summed[:, FP // 2 :]).astype(jnp.bfloat16)
    for y in range(N_Y):
        for low in range(N_F // 2):
            out_ref[y, :, WIDE * low : WIDE * (low + 1)] = weights[8 * low : 8 * low + 8].astype(jnp.bfloat16)
        out_ref[y, :, D // 2 :] = prints


def lift(order_ref, line_ref, out_ref):
    for j in range(LINE // 256):
        moved = jnp.dot(
            order_ref[...], line_ref[:, 256 * j : 256 * j + 256], preferred_element_type=jnp.float32
        ).astype(jnp.bfloat16)
        for h in range(2):
            at = h * (D // 2) + 256 * j if j < D // 512 else D + 256 * h
            for l in range(LAYERS):
                r = (h * LAYERS + l) * TALL
                for x in range(N_X):
                    out_ref[x, l, :, at : at + 256] = moved[r : r + TALL]


def finish(full_ref, w_ref, f_ref, done_ref):
    copies = []
    for l in range(LAYERS):
        for x in range(N_X):
            rows = pl.ds(x * TALL, TALL)
            for part, (ref, columns) in enumerate(((w_ref, pl.ds(0, D)), (f_ref, pl.ds(D, FP)))):
                copies.append(
                    pltpu.make_async_copy(
                        full_ref.at[x, l, :, columns], ref.at[l, rows, :], done_ref.at[l, x, part]
                    )
                )
                copies[-1].start()
    for copy in copies:
        copy.wait()


def shape_of(*dims):
    return jax.ShapeDtypeStruct(dims, jnp.bfloat16)


VMEM = pl.BlockSpec(memory_space=pltpu.VMEM)
SMEM = pl.BlockSpec(memory_space=pltpu.SMEM)


def regrouped(w):
    return pl.pallas_call(
        regroup,
        in_specs=[VMEM],
        out_specs=VMEM,
        out_shape=shape_of(N_Y, N_X, N_F * C, WIDE),
        name="regroup",
        compiler_params=pltpu.CompilerParams(vmem_limit_bytes=8 * 2**20),
    )(w.reshape(N_F, N_X, TALL, WIDE))


def picked(owner_k, got, centered):
    spot = np.arange(128)
    order = selection(spot // 4 % 2 * 64 + spot // 2 % 2 * 32 + spot // 8 * 2 + spot % 2, 128)
    return pl.pallas_call(
        pick,
        in_specs=[SMEM, VMEM, VMEM, VMEM],
        out_specs=VMEM,
        out_shape=shape_of(N_ZH, 128, WIDE),
        name="pick",
        compiler_params=pltpu.CompilerParams(vmem_limit_bytes=8 * 2**20),
    )(owner_k, order, got, centered)


def settled(owner_zh, recv):
    return pl.pallas_call(
        settle,
        in_specs=[SMEM, VMEM],
        out_specs=VMEM,
        out_shape=shape_of(N_Y, 8, LINE),
        name="settle",
        compiler_params=pltpu.CompilerParams(vmem_limit_bytes=6 * 2**20),
    )(owner_zh, recv)


def lifted(line):
    spot = np.arange(64)
    order = selection(spot // 2 % 8 * 8 + spot // 32 * 4 + spot // 16 % 2 * 2 + spot % 2, 64)
    return pl.pallas_call(
        lift,
        in_specs=[VMEM, VMEM],
        out_specs=VMEM,
        out_shape=shape_of(N_X, LAYERS, TALL, D + FP),
        name="lift",
        compiler_params=pltpu.CompilerParams(vmem_limit_bytes=8 * 2**20),
    )(order, line)


def finished(full):
    return pl.pallas_call(
        finish,
        in_specs=[VMEM],
        out_specs=[pl.BlockSpec(memory_space=pltpu.HBM)] * 2,
        out_shape=[shape_of(LAYERS, ROWS, D), shape_of(LAYERS, ROWS, FP)],
        scratch_shapes=[pltpu.SemaphoreType.DMA((LAYERS, N_X, 2))],
        name="finish",
        compiler_params=pltpu.CompilerParams(vmem_limit_bytes=8 * 2**20),
    )(full)


def solution(mesh):
    fine = Mesh(
        mesh.devices.reshape(N_ZL, N_CO, N_Y, N_ZH, N_X), ("zl", "co", "y", "zh", "x")
    )

    def body(w, table, assign):
        got = lax.all_to_all(
            regrouped(w).reshape(N_K, N_F * C, WIDE), ("y", "x"), 0, 0, tiled=True
        )
        centered = (table - 125).astype(jnp.bfloat16)
        owner_zh = assign // N_X % N_ZH
        owner_k = assign // (N_ZH * N_X) * N_X + assign % N_X
        send = picked(owner_k, got, centered)
        recv = lax.all_to_all(
            send.reshape(N_ZH * N_F, 8, WIDE), ("zh", "zl", "co"), 0, 0, tiled=True
        )
        lines = settled(owner_zh, recv.reshape(N_ZH * 128, WIDE))
        by_y = lax.all_to_all(lines, "y", 0, 0, tiled=True)
        full = lax.all_to_all(lifted(by_y.reshape(64, LINE)), "x", 0, 0, tiled=True)
        w_out, f_out = finished(full)
        return w_out[None], f_out[None]

    roll = ("y", "zh", "x")
    fsdp = ("zl", "co")
    return jax.shard_map(
        body, mesh=fine, in_specs=(P(roll, None, fsdp), P(fsdp, None), P(None)),
        out_specs=(P(roll, None, fsdp, None), P(roll, None, fsdp, None)), check_vma=False,
    )
```
